32 devices in a mesh: seq: 4 (over y, x), fsdp: 8 (over z, core).
Axes of the slice: x: 2, y: 2, z: 4, core: 2. Of those that a mesh axis runs over, the one named last changes fastest.
Arguments:
- tokens: bfloat16 [8, 512, 8192], P('fsdp', 'seq'), may hold values from -6 to 6
- norm_gain: float32 [8192], replicated, may hold values from 0.3 to 3
- w_query: bfloat16 [8192, 4096], P(('seq', 'fsdp')), may hold values from -1 to 1
- key_weight: bfloat16 [8192, 512], P(('seq', 'fsdp')), may hold values from -1 to 1
- value_weight: bfloat16 [8192, 512], P(('seq', 'fsdp')), may hold values from -0.0625 to 0.0625
- w_out: bfloat16 [4096, 8192], P(None, ('seq', 'fsdp')), may hold values from -0.09375 to 0.09375
Outputs:
- result: float32 [8, 512, 8192], P('fsdp', 'seq')
The draws below stay inside these ranges and needn't reach their ends.
All inputs are finite; a program needn't handle non-finite values.
Results may differ from the reference program's by a relative error of at most 0.04.
Values may be sent and summed in bfloat16 or wider, within the bound.
A program may use at most 128 MiB of HBM per device.

```python
import math
import jax
import jax.numpy as jnp
from jax import lax

MODEL_WIDTH = 8192
HQ = 32
KEY_VALUE_HEADS = 4
HEAD_SIZE = 128
GROUP = 8
SEQUENCE_TOKENS = 512
SEQS = 8
N_SEQ = 4


def projection_sample(key, head_count):
    normal_draw = jax.random.normal(jax.random.fold_in(key, 11), (MODEL_WIDTH, head_count * HEAD_SIZE), jnp.float32)
    normal_draw = jnp.clip(normal_draw, -6.0, 6.0) / math.sqrt(MODEL_WIDTH)
    normal_draw = jnp.clip(normal_draw, -1.0, 1.0)
    return normal_draw.astype(jnp.bfloat16)


def draw_w_query(key, part):
    return projection_sample(jax.random.fold_in(key, 101), HQ)


def draw_key_weight(key, part):
    return projection_sample(jax.random.fold_in(key, 202), KEY_VALUE_HEADS)


def shard_levels(rng, extent, split, smallest, top_value):
    def one(position, parts):
        heights = jax.random.uniform(jax.random.fold_in(jax.random.fold_in(rng, 6), position), (parts,), jnp.float32, smallest / len(split), top_value / len(split))
        return jnp.repeat(jnp.exp(heights), extent[position] // parts).reshape((-1,) + (1,) * (len(extent) - position - 1))

    level = one(*split[0])
    for cut in split[1:]:
        level = level * one(*cut)
    return level


def bell_draw(own_key, extent, deviation, bound, shards=(), kind=jnp.bfloat16):
    entries = jax.random.normal(own_key, extent, jnp.float32) * deviation
    if len(shards) > 0:
        entries = shard_levels(own_key, extent, shards, -0.22, 0.18) * entries
    return jnp.clip(entries, min=-bound, max=bound).astype(kind)


def setup_inputs(seed: int = 0) -> dict:
    splits = jax.random.split(jax.random.key(seed), 7)
    tokens = bell_draw(splits[0], (SEQS, SEQUENCE_TOKENS, MODEL_WIDTH), 1.0, 6.0, ((0, 8), (1, 4)))
    norm_gain = jnp.clip(jnp.exp(jax.random.uniform(splits[1], (MODEL_WIDTH,), jnp.float32, math.log(0.3), math.log(3.0))), 0.3, 3.0)
    w_query = draw_w_query(jax.random.fold_in(splits[6], 71), 0)
    key_weight = draw_key_weight(jax.random.fold_in(splits[6], 71), 0)
    value_weight = bell_draw(splits[4], (MODEL_WIDTH, KEY_VALUE_HEADS * HEAD_SIZE), MODEL_WIDTH ** -0.5, 0.0625, ((0, 32),))
    w_out = bell_draw(splits[5], (HQ * HEAD_SIZE, MODEL_WIDTH), (HQ * HEAD_SIZE) ** -0.5, 0.09375, ((1, 32),))
    return {"tokens": tokens, "norm_gain": norm_gain, "w_query": w_query, "key_weight": key_weight, "value_weight": value_weight, "w_out": w_out}


def rms_norm(sequence_rows, norm_gain):
    floats = sequence_rows.astype(jnp.float32)
    mean_square = lax.optimization_barrier(jnp.mean(floats * floats, axis=-1, keepdims=True))
    return (floats * lax.rsqrt(mean_square + 1e-05) * norm_gain).astype(jnp.bfloat16)

def apply_projection(normed_input, weight):
    block = MODEL_WIDTH // N_SEQ
    running = jnp.zeros((normed_input.shape[0], weight.shape[1]), jnp.float32)
    for block_index in range(N_SEQ):
        partial_sum = jnp.dot(normed_input[:, block_index * block:(block_index + 1) * block], weight[block_index * block:(block_index + 1) * block], preferred_element_type=jnp.float32)
        rounded = lax.optimization_barrier(partial_sum.astype(jnp.bfloat16))
        running = running + rounded.astype(jnp.float32)
    return running.astype(jnp.bfloat16)

def reference(tokens, norm_gain, w_query, key_weight, value_weight, w_out):
    scale = HEAD_SIZE ** (-0.5)
    row_ids = lax.broadcasted_iota(jnp.int32, (SEQUENCE_TOKENS, SEQUENCE_TOKENS), 0)
    col_ids = lax.broadcasted_iota(jnp.int32, (SEQUENCE_TOKENS, SEQUENCE_TOKENS), 1)
    causal = row_ids >= col_ids

    def one_sequence(sequence_rows):
        normed_input = rms_norm(sequence_rows, norm_gain)
        queries = apply_projection(normed_input, w_query).reshape(SEQUENCE_TOKENS, HQ, HEAD_SIZE)
        key_tensor = apply_projection(normed_input, key_weight).reshape(SEQUENCE_TOKENS, KEY_VALUE_HEADS, HEAD_SIZE)
        value_tensor = apply_projection(normed_input, value_weight).reshape(SEQUENCE_TOKENS, KEY_VALUE_HEADS, HEAD_SIZE)

        def one_head(head_index):
            query_head = lax.dynamic_index_in_dim(queries, head_index, 1, keepdims=False)
            kv_index = head_index // GROUP
            key_head = lax.dynamic_index_in_dim(key_tensor, kv_index, 1, keepdims=False)
            value_head = lax.dynamic_index_in_dim(value_tensor, kv_index, 1, keepdims=False)
            scores = jnp.dot(query_head, key_head.T, preferred_element_type=jnp.float32) * scale
            scores = jnp.where(causal, scores, jnp.float32(-1e+30))
            top = lax.optimization_barrier(jnp.max(scores, axis=-1, keepdims=True))
            weights = jnp.exp(scores - top)
            probs = (weights / lax.optimization_barrier(jnp.sum(weights, axis=-1, keepdims=True))).astype(jnp.bfloat16)
            return jnp.dot(probs, value_head, preferred_element_type=jnp.float32).astype(jnp.bfloat16)
        heads = lax.map(one_head, jnp.arange(HQ, dtype=jnp.int32))
        heads = jnp.transpose(heads, (1, 0, 2)).reshape(SEQUENCE_TOKENS, HQ * HEAD_SIZE)
        branch = jnp.dot(heads, w_out, preferred_element_type=jnp.float32).astype(jnp.bfloat16)
        return sequence_rows.astype(jnp.float32) + branch.astype(jnp.float32)
    return lax.map(one_sequence, tokens)
```

```python
import jax
import jax.numpy as jnp
from jax import lax
from jax.sharding import PartitionSpec as P

HEAD_SIZE = 128


def cut(array, start, size, axis):
    return lax.dynamic_slice_in_dim(array, start, size, axis)


def slot_table(stops):
    table = []
    for slot in range(1, stops):
        row = []
        for stop in range(stops):
            if stop < stops // 2:
                far, side, other = stops - 1 - stop, 1, -1
            else:
                far, side, other = stop, -1, 1
            row.append((side, slot) if slot <= far else (other, slot - far))
        table.append(row)
    return table


def line_steps(block, cores, meanwhile):
    devices = lax.axis_size("fsdp")
    stops = devices // cores
    arrived = {}
    for side in (1, -1):
        moving = block
        for step in range(1, stops):
            pairs = []
            for device in range(devices):
                target = device - side * cores
                source_stop = device // cores
                holds = source_stop + side * (step - 1)
                if 0 <= target < devices and 0 <= holds < stops:
                    pairs.append((device, target))
            if step in meanwhile:
                moving, _ = lax.optimization_barrier((moving, meanwhile[step]))
            moving = lax.ppermute(moving, "fsdp", pairs)
            arrived[(side, step)] = moving
    return arrived


def line_gather(block, cores, stop, meanwhile, before_last):
    devices = lax.axis_size("fsdp")
    stops = devices // cores
    arrived = line_steps(block, cores, meanwhile)
    swap = [(device, device ^ 1) for device in range(devices)]
    slots = [(stop, block, lax.ppermute(block, "fsdp", swap))]
    early = None
    for row in slot_table(stops):
        if len(slots) == stops - 1:
            early = before_last(slots)
            for side in (1, -1):
                arrived[(side, stops - 1)], early = lax.optimization_barrier(
                    (arrived[(side, stops - 1)], early)
                )
        chosen = None
        for key in sorted(set(row)):
            if chosen is None:
                chosen = arrived[key]
            else:
                here = jnp.bool_(False)
                for place, entry in enumerate(row):
                    if entry == key:
                        here = here | (stop == place)
                chosen = jnp.where(here, arrived[key], chosen)
        origin = jnp.int32(0)
        for place, (side, distance) in enumerate(row):
            origin = jnp.where(stop == place, place + side * distance, origin)
        slots.append((origin, chosen, lax.ppermute(chosen, "fsdp", swap)))
    return early, slots[-1]


def body(tokens, norm_gain, w_query, key_weight, value_weight, w_out):
    cores = 2
    group_size = lax.axis_size("seq")
    devices = lax.axis_size("fsdp")
    seq_index = lax.axis_index("seq")
    fsdp_index = lax.axis_index("fsdp")
    stop, core = fsdp_index // cores, fsdp_index % cores
    own_tokens = tokens[0]
    count, features = own_tokens.shape
    width = features // group_size
    depth = width // devices
    query_heads = w_query.shape[1] // HEAD_SIZE
    key_heads = key_weight.shape[1] // HEAD_SIZE
    group_width = query_heads // key_heads
    local_heads = query_heads // group_size
    local_width = local_heads * HEAD_SIZE
    seq_length = count * group_size

    def exchange(array, k):
        return lax.ppermute(array, "seq", [(i, i ^ k) for i in range(group_size)])

    columns = []
    for target in range(group_size):
        head = target * local_heads // group_width * HEAD_SIZE
        columns.append(w_query[:, target * local_width : (target + 1) * local_width])
        columns.append(key_weight[:, head : head + HEAD_SIZE])
        columns.append(value_weight[:, head : head + HEAD_SIZE])
    packed = jnp.concatenate(columns, axis=1)
    share = local_width + 2 * HEAD_SIZE
    floats = own_tokens.astype(jnp.float32)
    mean_square = jnp.mean(floats * floats, axis=-1, keepdims=True)
    normed = (floats * lax.rsqrt(mean_square + 1e-05) * norm_gain).astype(jnp.bfloat16)
    spread = jnp.zeros((seq_length, width), jnp.bfloat16)
    for k in range(group_size):
        piece = cut(normed, (seq_index ^ k) * width, width, 1)
        if k:
            piece = exchange(piece, k)
        spread = lax.dynamic_update_slice_in_dim(spread, piece, (seq_index ^ k) * count, 0)

    def features_of(origin, which):
        return cut(spread, (origin * cores + which) * depth, depth, 1)

    def mm(a, b):
        return jnp.dot(a, b, preferred_element_type=jnp.float32)

    def sum_of(slots):
        parts, blocks = [], []
        for origin, mine, other in slots:
            parts += [features_of(origin, core), features_of(origin, 1 - core)]
            blocks += [mine, other]
        return mm(jnp.concatenate(parts, 1), jnp.concatenate(blocks, 0))

    total, (origin, mine, other) = line_gather(packed, cores, stop, {2: spread}, sum_of)
    both = jnp.concatenate([features_of(origin, core), features_of(origin, 1 - core)], 1)
    last = jnp.concatenate([mine, other], 0)
    summed = None
    for k in list(range(group_size - 1, 0, -1)) + [0]:
        begin = (seq_index ^ k) * share
        part = mm(both, cut(last, begin, share, 1)) + cut(total, begin, share, 1)
        part = part.astype(jnp.bfloat16)
        if k:
            part = exchange(part, k)
        part = part.astype(jnp.float32)
        summed = part if summed is None else summed + part
    projected = summed.astype(jnp.bfloat16)

    queries = projected[:, :local_width].reshape(seq_length, local_heads, HEAD_SIZE)
    queries = jnp.transpose(queries, (1, 0, 2))
    key_rows = projected[:, local_width : local_width + HEAD_SIZE]
    value_rows = projected[:, local_width + HEAD_SIZE :]
    scale = HEAD_SIZE ** (-0.5)
    row_ids = lax.broadcasted_iota(jnp.int32, (seq_length, seq_length), 0)
    col_ids = lax.broadcasted_iota(jnp.int32, (seq_length, seq_length), 1)
    causal = row_ids >= col_ids

    def one_head(query_head):
        scores = (
            jnp.einsum("qd,kd->qk", query_head, key_rows, preferred_element_type=jnp.float32)
            * scale
        )
        scores = jnp.where(causal, scores, jnp.float32(-1e30))
        top = jnp.max(scores, axis=-1, keepdims=True)
        weights = jnp.exp(scores - top)
        probs = (weights / jnp.sum(weights, axis=-1, keepdims=True)).astype(jnp.bfloat16)
        return jnp.dot(probs, value_rows, preferred_element_type=jnp.float32).astype(jnp.bfloat16)

    attended = lax.map(one_head, queries)
    heads_own = jnp.transpose(attended, (1, 0, 2)).reshape(seq_length, local_width)
    heads = jnp.zeros((seq_length, query_heads * HEAD_SIZE), jnp.bfloat16)
    for k in range(group_size):
        piece = exchange(heads_own, k) if k else heads_own
        heads = lax.dynamic_update_slice_in_dim(heads, piece, (seq_index ^ k) * local_width, 1)

    held, _ = lax.optimization_barrier((w_out, mine))

    def add_branches(branches, slot):
        origin, mine, other = slot
        first, second = mm(heads, mine), mm(heads, other)
        branch = jnp.where(
            core == 0,
            jnp.concatenate([first, second], 1),
            jnp.concatenate([second, first], 1),
        ).astype(jnp.bfloat16)
        for k in range(group_size):
            piece = cut(branch, (seq_index ^ k) * count, count, 0)
            if k:
                piece = exchange(piece, k)
            begin = ((seq_index ^ k) * devices + origin * cores) * depth
            branches = lax.dynamic_update_slice_in_dim(branches, piece, begin, 1)
        return branches

    def branches_of(slots):
        branches = jnp.zeros((count, features), jnp.bfloat16)
        for slot in slots:
            branches = add_branches(branches, slot)
        return branches

    early, slot = line_gather(held, cores, stop, {3: heads_own}, branches_of)
    branches = add_branches(early, slot)
    return tokens.astype(jnp.float32) + branches[None].astype(jnp.float32)


def solution(mesh):
    placed = (
        P("fsdp", "seq", None),
        P(),
        P(("seq", "fsdp"), None),
        P(("seq", "fsdp"), None),
        P(("seq", "fsdp"), None),
        P(None, ("seq", "fsdp")),
    )
    return jax.shard_map(
        body, mesh=mesh, in_specs=placed, out_specs=P("fsdp", "seq", None), check_vma=False
    )
```

```python
import jax
import jax.numpy as jnp
from jax import lax
from jax.sharding import PartitionSpec as P

HEAD_SIZE = 128


def cut(array, start, size, axis):
    return lax.dynamic_slice_in_dim(array, start, size, axis)


def slot_table(stops):
    table = []
    for slot in range(1, stops):
        row = []
        for stop in range(stops):
            if stop < stops // 2:
                far, side, other = stops - 1 - stop, 1, -1
            else:
                far, side, other = stop, -1, 1
            row.append((side, slot) if slot <= far else (other, slot - far))
        table.append(row)
    return table


def line_steps(block, cores, meanwhile):
    devices = lax.axis_size("fsdp")
    stops = devices // cores
    arrived = {}
    for side in (1, -1):
        moving = block
        for step in range(1, stops):
            pairs = []
            for device in range(devices):
                target = device - side * cores
                holds = device // cores + side * (step - 1)
                if 0 <= target < devices and 0 <= holds < stops:
                    pairs.append((device, target))
            if step in meanwhile:
                moving, _ = lax.optimization_barrier((moving, meanwhile[step]))
            moving = lax.ppermute(moving, "fsdp", pairs)
            arrived[(side, step)] = moving
    return arrived


def line_gather(block, cores, stop, meanwhile, before_last):
    devices = lax.axis_size("fsdp")
    stops = devices // cores
    arrived = line_steps(block, cores, meanwhile)
    swap = [(device, device ^ 1) for device in range(devices)]
    slots = [(stop, block, lax.ppermute(block, "fsdp", swap))]
    early = None
    for row in slot_table(stops):
        if len(slots) == stops - 1:
            early = before_last(slots)
            for side in (1, -1):
                arrived[(side, stops - 1)], early = lax.optimization_barrier(
                    (arrived[(side, stops - 1)], early)
                )
        chosen = None
        for key in sorted(set(row)):
            if chosen is None:
                chosen = arrived[key]
            else:
                here = jnp.bool_(False)
                for place, entry in enumerate(row):
                    if entry == key:
                        here = here | (stop == place)
                chosen = jnp.where(here, arrived[key], chosen)
        origin = jnp.int32(0)
        for place, (side, distance) in enumerate(row):
            origin = jnp.where(stop == place, place + side * distance, origin)
        slots.append((origin, chosen, lax.ppermute(chosen, "fsdp", swap)))
    return early, slots[-1]


def body(tokens, norm_gain, w_query, key_weight, value_weight, w_out):
    cores = 2
    group_size = lax.axis_size("seq")
    devices = lax.axis_size("fsdp")
    seq_index = lax.axis_index("seq")
    fsdp_index = lax.axis_index("fsdp")
    stop, core = fsdp_index // cores, fsdp_index % cores
    own_tokens = tokens[0]
    count, features = own_tokens.shape
    width = features // group_size
    depth = width // devices
    query_heads = w_query.shape[1] // HEAD_SIZE
    key_heads = key_weight.shape[1] // HEAD_SIZE
    group_width = query_heads // key_heads
    local_heads = query_heads // group_size
    local_width = local_heads * HEAD_SIZE
    seq_length = count * group_size

    def exchange(array, k):
        return lax.ppermute(array, "seq", [(i, i ^ k) for i in range(group_size)])

    packed = jnp.concatenate([w_query, key_weight, value_weight], axis=1)
    query_width = query_heads * HEAD_SIZE
    key_width = key_heads * HEAD_SIZE

    floats = own_tokens.astype(jnp.float32)
    mean_square = jnp.mean(floats * floats, axis=-1, keepdims=True)
    normed = (floats * lax.rsqrt(mean_square + 1e-05) * norm_gain).astype(jnp.bfloat16)
    spread = jnp.zeros((seq_length, width), jnp.bfloat16)
    for k in range(group_size):
        piece = cut(normed, (seq_index ^ k) * width, width, 1)
        if k:
            piece = exchange(piece, k)
        spread = lax.dynamic_update_slice_in_dim(spread, piece, (seq_index ^ k) * count, 0)

    def features_of(origin, which):
        return cut(spread, (origin * cores + which) * depth, depth, 1)

    def mm(a, b):
        return jnp.dot(a, b, preferred_element_type=jnp.float32)

    def sum_of(slots):
        parts, blocks = [], []
        for origin, mine, other in slots:
            parts += [features_of(origin, core), features_of(origin, 1 - core)]
            blocks += [mine, other]
        return mm(jnp.concatenate(parts, 1), jnp.concatenate(blocks, 0))

    total, (origin, mine, other) = line_gather(packed, cores, stop, {2: spread}, sum_of)
    both = jnp.concatenate([features_of(origin, core), features_of(origin, 1 - core)], 1)
    last = jnp.concatenate([mine, other], 0)
    pair_part = mm(both, last[:, query_width:]) + total[:, query_width:]
    pair_part = pair_part.astype(jnp.bfloat16)
    pair_sum, query_sum = None, None
    for k in list(range(group_size - 1, 0, -1)) + [0]:
        target = seq_index ^ k
        head = target * local_heads // group_width * HEAD_SIZE
        pair = jnp.concatenate(
            [cut(pair_part, head, HEAD_SIZE, 1), cut(pair_part, key_width + head, HEAD_SIZE, 1)], 1
        )
        begin = target * local_width
        query = mm(both, cut(last, begin, local_width, 1)) + cut(total, begin, local_width, 1)
        query = query.astype(jnp.bfloat16)
        if k:
            pair, query = exchange(pair, k), exchange(query, k)
        pair, query = pair.astype(jnp.float32), query.astype(jnp.float32)
        pair_sum = pair if pair_sum is None else pair_sum + pair
        query_sum = query if query_sum is None else query_sum + query
    pair_sum = pair_sum.astype(jnp.bfloat16)

    queries = query_sum.astype(jnp.bfloat16).reshape(seq_length, local_heads, HEAD_SIZE)
    queries = jnp.transpose(queries, (1, 0, 2))
    key_rows = pair_sum[:, :HEAD_SIZE]
    value_rows = pair_sum[:, HEAD_SIZE:]
    scale = HEAD_SIZE ** (-0.5)
    row_ids = lax.broadcasted_iota(jnp.int32, (seq_length, seq_length), 0)
    col_ids = lax.broadcasted_iota(jnp.int32, (seq_length, seq_length), 1)
    causal = row_ids >= col_ids

    def one_head(query_head):
        scores = (
            jnp.einsum("qd,kd->qk", query_head, key_rows, preferred_element_type=jnp.float32)
            * scale
        )
        scores = jnp.where(causal, scores, jnp.float32(-1e30))
        top = jnp.max(scores, axis=-1, keepdims=True)
        weights = jnp.exp(scores - top)
        probs = (weights / jnp.sum(weights, axis=-1, keepdims=True)).astype(jnp.bfloat16)
        return jnp.dot(probs, value_rows, preferred_element_type=jnp.float32).astype(jnp.bfloat16)

    attended = lax.map(one_head, queries)
    heads_own = jnp.transpose(attended, (1, 0, 2)).reshape(seq_length, local_width)
    heads = jnp.zeros((seq_length, query_heads * HEAD_SIZE), jnp.bfloat16)
    for k in range(group_size):
        piece = exchange(heads_own, k) if k else heads_own
        heads = lax.dynamic_update_slice_in_dim(heads, piece, (seq_index ^ k) * local_width, 1)

    held, _ = lax.optimization_barrier((w_out, mine))

    def add_branches(branches, slot):
        origin, mine, other = slot
        first, second = mm(heads, mine), mm(heads, other)
        branch = jnp.where(
            core == 0,
            jnp.concatenate([first, second], 1),
            jnp.concatenate([second, first], 1),
        ).astype(jnp.bfloat16)
        for k in range(group_size):
            piece = cut(branch, (seq_index ^ k) * count, count, 0)
            if k:
                piece = exchange(piece, k)
            begin = ((seq_index ^ k) * devices + origin * cores) * depth
            branches = lax.dynamic_update_slice_in_dim(branches, piece, begin, 1)
        return branches

    def branches_of(slots):
        branches = jnp.zeros((count, features), jnp.bfloat16)
        for slot in slots:
            branches = add_branches(branches, slot)
        return branches

    early, slot = line_gather(held, cores, stop, {3: heads_own}, branches_of)
    branches = add_branches(early, slot)
    return tokens.astype(jnp.float32) + branches[None].astype(jnp.float32)


def solution(mesh):
    placed = (
        P("fsdp", "seq", None),
        P(),
        P(("seq", "fsdp"), None),
        P(("seq", "fsdp"), None),
        P(("seq", "fsdp"), None),
        P(None, ("seq", "fsdp")),
    )
    return jax.shard_map(
        body, mesh=mesh, in_specs=placed, out_specs=P("fsdp", "seq", None), check_vma=False
    )
```
